32 devices in a mesh: expert: 16 (over z, y, x), width: 2 (over core).
Axes of the slice: x: 2, y: 2, z: 4, core: 2. Of those that a mesh axis runs over, the one named last changes fastest.
Arguments:
- tokens: bfloat16 [1024, 6144], P('expert', 'width'), may hold values from -6 to 6
- expert_ids: int32 [1024, 8], P('expert'), may hold values from 0 to 383, all different within a row; in each aligned block of 64 rows (0 to 63, 64 to 127, ...) at most 2 rows name the same one
- route_weight: float32 [1024, 8], P('expert'), may hold values from 0.2 to 1.5
- gate_weight: bfloat16 [16, 6144, 1024], P('expert', None, 'width'), may hold values from -0.078125 to 0.078125
- up_weight: bfloat16 [16, 6144, 1024], P('expert', None, 'width'), may hold values from -0.078125 to 0.078125
- down_weight: bfloat16 [16, 6144, 1024], P('expert', None, 'width'), may hold values from -0.1875 to 0.1875
Outputs:
- mixed: bfloat16 [1024, 6144], P('expert', 'width')
The draws below stay inside these ranges and needn't reach their ends.
Inputs may be any that keep to these rules, and one draw needn't show every extreme that they name: `expert_ids`: each row names 8 different experts. In each aligned block of 64 rows (the rows of one index of the expert axis) no expert is named by more than 2 rows.
All inputs are finite; a program needn't handle non-finite values.
Results may differ from the reference program's by a relative error of at most 0.014.
Values may be sent and summed in bfloat16 or wider, within the bound.
No kernel may reach another device: no remote copies, remote signals or barrier semaphores. Data moves between devices by JAX's collectives and lax.ppermute only.
A program may use at most 64 MiB of HBM per device.

```python
import math
import jax
import jax.numpy as jnp
import numpy as np
from jax import lax

D = 6144
FF = 1024
EXPERTS = 384
TOPK = 8
TOK_DEV = 64
SEND = 2
HELD = 16
TOKENS = 1024
N_WIDTH = 2


def block_levels(stream_key, extent, split, least, top_value):
    level, own = 1.0, jax.random.fold_in(stream_key, 6)
    for axis_at, blocks in split:
        steps = jnp.exp(jax.random.uniform(jax.random.fold_in(own, axis_at), (blocks,), jnp.float32, least / len(split), top_value / len(split)))
        level = level * jnp.repeat(steps, extent[axis_at] // blocks).reshape([-1 if axis == axis_at else 1 for axis in range(len(extent))])
    return level


def shared_out(stream_key, own, number, rows, count, top, bound, skew):
    order = jax.random.permutation(stream_key, count)
    packed, usual = load_shares(count, rows * top, bound, skew, True), load_shares(count, rows * top, bound, skew, False)
    places = jnp.arange(count)

    def named(tallies, turn):
        used = int((tallies > 0).sum())
        fixed = max(1, used // 4)
        moved = fixed + (places - fixed + turn * (used - fixed)) % max(1, count - fixed)
        return jnp.zeros((count,), jnp.int32).at[order[jnp.where(places < fixed, places, moved)]].set(jnp.asarray(tallies, jnp.int32))

    tallies = jnp.where(number % 4 == 0, named(packed, number // 4), named(usual, number - number // 4 - 1))
    mixed = jax.random.permutation(jax.random.fold_in(own, 3), count)
    source_of, taker = mixed[0:count // 2 * 2:2], mixed[1:count // 2 * 2:2]
    slack = jnp.minimum(tallies[source_of] - 1, bound - tallies[taker]) // 2
    slack = jnp.where((source_of == order[0]) | (taker == order[0]) | (tallies[taker] == 0), 0, jnp.maximum(slack, 0))
    moved = jax.random.randint(jax.random.fold_in(own, 4), (count // 2,), 0, 1 << 20) % (slack + 1)
    tallies = tallies.at[source_of].add(-moved).at[taker].add(moved)
    items = jnp.searchsorted(jnp.cumsum(tallies), jnp.arange(rows * top), side="right").astype(jnp.int32)
    table = items.reshape(top, rows).T
    table = table[jax.random.permutation(jax.random.fold_in(own, 1), rows)]
    turn = jax.random.randint(jax.random.fold_in(own, 2), (rows, 1), 0, top)
    return jnp.take_along_axis(table, (jnp.arange(top)[None, :] + turn) % top, axis=1)


def load_shares(count, total, bound, lean, full):
    loads = [(1 << 20) // math.isqrt(standing ** lean) + 1 for standing in range(1, count + 1)]
    largest = bound if full else min(bound, max(-(-total // count), total * loads[0] // sum(loads)))
    least = 1 if total - largest >= count - 1 else 0
    holding, surplus = [largest] + [least] * (count - 1), total - largest - least * (count - 1)
    while surplus > 0:
        candidates = [i for i in range(1, count) if holding[i] < largest] or [i for i in range(1, count) if holding[i] < bound]
        pool, remaining = sum([loads[i] for i in candidates]), surplus
        for i in candidates:
            more = min(bound - holding[i], max(1, remaining * loads[i] // pool), surplus)
            holding[i] = holding[i] + more
            surplus = surplus - more
    return np.array(holding)


def noise(stream_key, dims, spread, most, split=(), held_as=jnp.bfloat16):
    level = block_levels(stream_key, dims, split, -0.22, 0.18) if split else 1.0
    drawn = jax.random.normal(stream_key, dims, jnp.float32) * spread * level
    return jnp.minimum(jnp.maximum(drawn, -most), most).astype(held_as)


def setup_inputs(seed: int = 0) -> dict:
    arg_keys = jax.random.split(jax.random.key(seed), 7)
    tokens = noise(arg_keys[0], (TOKENS, D), 1.0, 6.0, ((0, 16), (1, 2)))
    expert_ids_keys = jax.random.split(jax.random.fold_in(arg_keys[1], 1), TOKENS // TOK_DEV)
    expert_ids_turns = jax.random.permutation(jax.random.fold_in(arg_keys[1], 3), TOKENS // TOK_DEV)
    expert_ids = jax.vmap(lambda own, number: shared_out(jax.random.fold_in(arg_keys[1], 2), own, number, TOK_DEV, EXPERTS, TOPK, SEND, 2))(expert_ids_keys, expert_ids_turns).reshape((TOKENS, TOPK))
    route_weight = jnp.clip(0.2 + 1.3 * jax.random.uniform(arg_keys[2], (TOKENS, TOPK), jnp.float32) ** block_levels(arg_keys[2], (TOKENS, TOPK), ((0, 16),), -0.2, 0.2), 0.2, 1.5)
    gate_weight = noise(arg_keys[3], (HELD, D, FF), D ** -0.5, 0.078125, ((0, 16), (2, 2)))
    up_weight = noise(arg_keys[4], (HELD, D, FF), D ** -0.5, 0.078125, ((0, 16), (2, 2)))
    down_weight = noise(arg_keys[5], (HELD, D, FF), FF ** -0.5, 0.1875, ((0, 16), (2, 2)))
    return {"tokens": tokens, "expert_ids": expert_ids, "route_weight": route_weight, "gate_weight": gate_weight, "up_weight": up_weight, "down_weight": down_weight}


def reference(tokens, expert_ids, route_weight, gate_weight, up_weight, down_weight):
    tokens_total = tokens.shape[0]
    capacity = HELD * SEND
    width_slice = FF // N_WIDTH
    block_count = tokens_total // TOK_DEV
    row_index = jnp.arange(tokens_total, dtype=jnp.int32)
    block_of = row_index // TOK_DEV

    def expert_step(expert, combined):
        route_hits = expert_ids == expert
        routed = jnp.any(route_hits, axis=1).astype(jnp.int32)
        blocked = routed.reshape(block_count, TOK_DEV)
        ranking = (jnp.cumsum(blocked, axis=1) - blocked).reshape(-1).astype(jnp.int32)
        slot_of = jnp.where(routed > 0, block_of * SEND + ranking, capacity).astype(jnp.int32)
        slot_table = jnp.full((capacity + 1,), tokens_total, jnp.int32).at[slot_of].set(row_index)[:capacity]
        selected = jnp.take(tokens, slot_table, axis=0, mode="fill", fill_value=0)
        gate_mat = lax.dynamic_index_in_dim(gate_weight, expert, 0, keepdims=False)
        up_mat = lax.dynamic_index_in_dim(up_weight, expert, 0, keepdims=False)
        down_mat = lax.dynamic_index_in_dim(down_weight, expert, 0, keepdims=False)
        gate_val = jnp.dot(selected, gate_mat, preferred_element_type=jnp.float32)
        up_val = jnp.dot(selected, up_mat, preferred_element_type=jnp.float32)
        hidden = (jax.nn.silu(gate_val) * up_val).astype(jnp.bfloat16)
        expert_out = jnp.zeros((capacity, D), jnp.float32)
        for section in range(N_WIDTH):
            lower = section * width_slice
            part = lax.dot_general(hidden[:, lower:lower + width_slice], down_mat[:, lower:lower + width_slice],
                                   (((1,), (1,)), ((), ())), preferred_element_type=jnp.float32)
            expert_out = expert_out + part.astype(jnp.bfloat16).astype(jnp.float32)
        coeff = jnp.sum(jnp.where(route_hits, route_weight, jnp.zeros_like(route_weight)), axis=1)
        slot_coeff = jnp.take(coeff, slot_table, mode="fill", fill_value=0.0)
        return combined.at[slot_table].add(slot_coeff[:, None] * expert_out, mode="drop")

    combined = lax.fori_loop(0, HELD, expert_step, jnp.zeros((tokens_total, D), jnp.float32))
    return combined.astype(jnp.bfloat16)
```

```python
import functools

import jax
import jax.numpy as jnp
from jax import lax
from jax.experimental import pallas as pl
from jax.experimental.pallas import tpu as pltpu
from jax.sharding import PartitionSpec as P

SEND = 2
VMEM = pl.BlockSpec(memory_space=pltpu.VMEM)
F32 = jnp.float32
BF16 = jnp.bfloat16


def params(mib):
    return pltpu.CompilerParams(vmem_limit_bytes=mib << 20)


def route_kernel(ids_ref, weight_ref, tokens_ref, outgoing_ref, coeff_ref):
    slots, rows = coeff_ref.shape
    slot = lax.broadcasted_iota(jnp.int32, (slots, rows), 0)
    expert, rank = slot // SEND, slot % SEND
    hits = jnp.zeros((slots, rows), F32)
    weight = jnp.zeros((slots, rows), F32)
    for k in range(ids_ref.shape[0]):
        hit = ids_ref[k : k + 1, :] == expert
        hits = jnp.where(hit, 1.0, hits)
        weight = jnp.where(hit, weight_ref[k : k + 1, :], weight)
    earlier = lax.broadcasted_iota(jnp.int32, (rows, rows), 0) < lax.broadcasted_iota(
        jnp.int32, (rows, rows), 1
    )
    ranking = jnp.dot(hits.astype(BF16), earlier.astype(BF16), preferred_element_type=F32)
    taken = jnp.logical_and(hits > 0.0, ranking == rank.astype(F32))
    coeff_ref[...] = jnp.where(taken, weight, 0.0)
    outgoing_ref[...] = jnp.dot(
        taken.astype(BF16), tokens_ref[...], preferred_element_type=F32
    ).astype(BF16)


def expert_kernel(width, *refs):
    rows = refs[:width]
    gate_ref, up_ref, down_ref = refs[width : width + 3]
    parts = refs[width + 3 :]
    features = rows[0].shape[1]
    me = lax.axis_index("width")
    gate = up = 0.0
    for d in range(width):
        block = pl.ds(pl.multiple_of(lax.rem(me + width - d, width) * features, features), features)
        x = rows[d][...]
        gate += jnp.dot(x, gate_ref[0, block, :], preferred_element_type=F32)
        up += jnp.dot(x, up_ref[0, block, :], preferred_element_type=F32)
    hidden = (gate / (1.0 + jnp.exp(-gate)) * up).astype(BF16)
    for d in range(width):
        block = pl.ds(pl.multiple_of(lax.rem(me + d, width) * features, features), features)
        parts[d][...] = lax.dot_general(
            hidden, down_ref[0, block, :], (((1,), (1,)), ((), ())), preferred_element_type=F32
        ).astype(BF16)


def combine_kernel(coeff_ref, returned_ref, mixed_ref):
    coeff = coeff_ref[...]
    high = coeff.astype(BF16)
    low = (coeff - high.astype(F32)).astype(BF16)
    returned = returned_ref[...]
    dims = (((0,), (0,)), ((), ()))
    mixed_ref[...] = (
        lax.dot_general(high, returned, dims, preferred_element_type=F32)
        + lax.dot_general(low, returned, dims, preferred_element_type=F32)
    ).astype(BF16)


def body(tokens, expert_ids, route_weight, gate_weight, up_weight, down_weight):
    holders, width = lax.axis_size("expert"), lax.axis_size("width")
    rows, features = tokens.shape
    slots = holders * SEND
    outgoing, coeff = pl.pallas_call(
        route_kernel,
        out_shape=(
            jax.ShapeDtypeStruct((slots, features), BF16),
            jax.ShapeDtypeStruct((slots, rows), F32),
        ),
        in_specs=[VMEM] * 3,
        out_specs=(VMEM, VMEM),
        compiler_params=params(8),
        name="route",
    )(expert_ids.T, route_weight.T, tokens)

    def exchange(x):
        return lax.all_to_all(
            x.reshape(holders, SEND, features), "expert", split_axis=0, concat_axis=0, tiled=True
        ).reshape(slots, features)

    def shifted(x, d):
        return lax.ppermute(x, "width", [(i, (i + d) % width) for i in range(width)])

    arrived = exchange(outgoing)
    blocks = [arrived] + [shifted(arrived, d) for d in range(1, width)]
    weights = [
        pltpu.with_memory_space_constraint(w, pltpu.VMEM)
        for w in (gate_weight, up_weight, down_weight)
    ]
    parts = pl.pallas_call(
        functools.partial(expert_kernel, width),
        out_shape=[jax.ShapeDtypeStruct((slots, features), BF16)] * width,
        in_specs=[VMEM] * (width + 3),
        out_specs=[VMEM] * width,
        compiler_params=params(24),
        name="experts",
    )(*blocks, *weights)
    summed = parts[0].astype(F32)
    for d in range(1, width):
        summed = summed + shifted(parts[d], d).astype(F32)
    returned = exchange(summed.astype(BF16))
    return pl.pallas_call(
        combine_kernel,
        out_shape=jax.ShapeDtypeStruct((rows, features), BF16),
        in_specs=[VMEM] * 2,
        out_specs=VMEM,
        compiler_params=params(8),
        name="combine",
    )(coeff, returned)


def solution(mesh):
    in_specs = (
        P("expert", "width"),
        P("expert", None),
        P("expert", None),
        P("expert", None, "width"),
        P("expert", None, "width"),
        P("expert", None, "width"),
    )
    out_specs = P("expert", "width")
    return jax.shard_map(body, mesh=mesh, in_specs=in_specs, out_specs=out_specs, check_vma=False)
```

```python
import functools

import jax
import jax.numpy as jnp
from jax import lax
from jax.experimental import pallas as pl
from jax.experimental.pallas import tpu as pltpu
from jax.sharding import PartitionSpec as P

SEND = 2
VMEM = pl.BlockSpec(memory_space=pltpu.VMEM)
HBM = pl.BlockSpec(memory_space=pltpu.HBM)
F32 = jnp.float32
BF16 = jnp.bfloat16


def params(mib):
    return pltpu.CompilerParams(vmem_limit_bytes=mib << 20)


def hint(micros):
    return pl.CostEstimate(flops=micros * 10**9, bytes_accessed=0, transcendentals=0)


def split_rows(ref, value):
    for e in range(ref.shape[0]):
        ref[e] = value[e * SEND : (e + 1) * SEND, :]


def join_rows(ref):
    return jnp.concatenate([ref[e] for e in range(ref.shape[0])], axis=0)


def slots_kernel(ids_hbm, weight_hbm, tokens_hbm, taken_ref, coeff_ref, tokens_ref, ids_ref, weight_ref, sems):
    copies = [
        pltpu.make_async_copy(source, target, sems.at[i])
        for i, (source, target) in enumerate(
            ((ids_hbm, ids_ref), (weight_hbm, weight_ref), (tokens_hbm, tokens_ref))
        )
    ]
    for copy in copies:
        copy.start()
    slots, rows = coeff_ref.shape
    slot = lax.broadcasted_iota(jnp.int32, (slots, rows), 0)
    expert, rank = slot // SEND, slot % SEND
    earlier = lax.broadcasted_iota(jnp.int32, (rows, rows), 0) < lax.broadcasted_iota(
        jnp.int32, (rows, rows), 1
    )
    hits = jnp.zeros((slots, rows), F32)
    weight = jnp.zeros((slots, rows), F32)
    copies[0].wait()
    copies[1].wait()
    for k in range(ids_ref.shape[0]):
        hit = ids_ref[k : k + 1, :] == expert
        hits = jnp.where(hit, 1.0, hits)
        weight = jnp.where(hit, weight_ref[k : k + 1, :], weight)
    ranking = jnp.dot(hits.astype(BF16), earlier.astype(BF16), preferred_element_type=F32)
    taken = jnp.logical_and(hits > 0.0, ranking == rank.astype(F32))
    coeff_ref[...] = jnp.where(taken, weight, 0.0)
    taken_ref[...] = jnp.where(taken, 1.0, 0.0).astype(BF16)
    copies[2].wait()


def select_kernel(taken_ref, tokens_ref, outgoing_ref):
    split_rows(
        outgoing_ref,
        jnp.dot(taken_ref[...], tokens_ref[...], preferred_element_type=F32).astype(BF16),
    )


def feature_block(d, features):
    width = lax.axis_size("width")
    owner = lax.rem(lax.axis_index("width") + width - d, width)
    return pl.ds(pl.multiple_of(owner * features, features), features)


def own_kernel(rows_ref, gate_ref, up_ref, gate_out, up_out):
    x = join_rows(rows_ref)
    block = feature_block(0, x.shape[1])
    gate_out[...] = jnp.dot(x, gate_ref[0, block, :], preferred_element_type=F32)
    up_out[...] = jnp.dot(x, up_ref[0, block, :], preferred_element_type=F32)


def down_block(hidden, down_ref, d, features):
    return lax.dot_general(
        hidden,
        down_ref[0, feature_block(d, features), :],
        (((1,), (1,)), ((), ())),
        preferred_element_type=F32,
    ).astype(BF16)


def others_kernel(others, *refs):
    rows = refs[:others]
    gate_in, up_in, gate_ref, up_ref, down_ref = refs[others : others + 5]
    hidden_ref = refs[others + 5]
    parts = refs[others + 6 :]
    gate, up = gate_in[...], up_in[...]
    for d in range(others):
        x = join_rows(rows[d])
        block = feature_block(d + 1, x.shape[1])
        gate += jnp.dot(x, gate_ref[0, block, :], preferred_element_type=F32)
        up += jnp.dot(x, up_ref[0, block, :], preferred_element_type=F32)
    hidden = (gate / (1.0 + jnp.exp(-gate)) * up).astype(BF16)
    hidden_ref[...] = hidden
    for d in range(others):
        parts[d][...] = down_block(hidden, down_ref, d + 1, parts[d].shape[1])


def own_part_kernel(hidden_ref, down_ref, part_ref):
    part_ref[...] = down_block(hidden_ref[...], down_ref, 0, part_ref.shape[1])


def combine_kernel(coeff_ref, returned_ref, mixed_ref):
    coeff = coeff_ref[...]
    high = coeff.astype(BF16)
    low = (coeff - high.astype(F32)).astype(BF16)
    returned = join_rows(returned_ref)
    dims = (((0,), (0,)), ((), ()))
    mixed_ref[...] = (
        lax.dot_general(high, returned, dims, preferred_element_type=F32)
        + lax.dot_general(low, returned, dims, preferred_element_type=F32)
    ).astype(BF16)


def body(tokens, expert_ids, route_weight, gate_weight, up_weight, down_weight):
    holders, width = lax.axis_size("expert"), lax.axis_size("width")
    rows, features = tokens.shape
    top = expert_ids.shape[1]
    hidden_units = gate_weight.shape[2]
    slots = holders * SEND
    shape = jax.ShapeDtypeStruct

    ids, weights, tokens = (
        pltpu.with_memory_space_constraint(x, pltpu.HBM)
        for x in (expert_ids.T, route_weight.T, tokens)
    )
    taken, coeff, tokens = pl.pallas_call(
        slots_kernel,
        out_shape=(
            shape((slots, rows), BF16),
            shape((slots, rows), F32),
            shape((rows, features), BF16),
        ),
        in_specs=[HBM] * 3,
        out_specs=[VMEM] * 3,
        scratch_shapes=[
            pltpu.VMEM((top, rows), jnp.int32),
            pltpu.VMEM((top, rows), F32),
            pltpu.SemaphoreType.DMA((3,)),
        ],
        compiler_params=params(8),
        name="slots",
    )(ids, weights, tokens)
    outgoing = pl.pallas_call(
        select_kernel,
        out_shape=shape((holders, SEND, features), BF16),
        in_specs=[VMEM] * 2,
        out_specs=VMEM,
        compiler_params=params(8),
        cost_estimate=hint(40),
        name="select",
    )(taken, tokens)

    def exchange(x):
        return lax.all_to_all(x, "expert", split_axis=0, concat_axis=0, tiled=True)

    def shifted(x, d):
        return lax.ppermute(x, "width", [(i, (i + d) % width) for i in range(width)])

    arrived = exchange(outgoing)
    others = [shifted(arrived, d) for d in range(1, width)]
    gate_vmem, up_vmem, down_vmem = (
        pltpu.with_memory_space_constraint(w, pltpu.VMEM)
        for w in (gate_weight, up_weight, down_weight)
    )
    gate, up = pl.pallas_call(
        own_kernel,
        out_shape=[shape((slots, hidden_units), F32)] * 2,
        in_specs=[VMEM] * 3,
        out_specs=[VMEM] * 2,
        compiler_params=params(20),
        cost_estimate=hint(2),
        name="own",
    )(arrived, gate_vmem, up_vmem)
    hidden, *parts = pl.pallas_call(
        functools.partial(others_kernel, width - 1),
        out_shape=[shape((slots, hidden_units), BF16)]
        + [shape((slots, features), BF16)] * (width - 1),
        in_specs=[VMEM] * (width + 4),
        out_specs=[VMEM] * width,
        compiler_params=params(24),
        cost_estimate=hint(2),
        name="others",
    )(*others, gate, up, gate_vmem, up_vmem, down_vmem)
    received = [shifted(part, d + 1) for d, part in enumerate(reversed(parts))]
    summed = pl.pallas_call(
        own_part_kernel,
        out_shape=shape((slots, features), BF16),
        in_specs=[VMEM] * 2,
        out_specs=VMEM,
        compiler_params=params(20),
        cost_estimate=hint(2),
        name="own_part",
    )(hidden, down_vmem).astype(F32)
    for part in received:
        summed = summed + part.astype(F32)
    returned = exchange(summed.astype(BF16).reshape(holders, SEND, features))
    return pl.pallas_call(
        combine_kernel,
        out_shape=shape((rows, features), BF16),
        in_specs=[VMEM] * 2,
        out_specs=VMEM,
        compiler_params=params(8),
        name="combine",
    )(coeff, returned)


def solution(mesh):
    in_specs = (
        P("expert", "width"),
        P("expert", None),
        P("expert", None),
        P("expert", None, "width"),
        P("expert", None, "width"),
        P("expert", None, "width"),
    )
    out_specs = P("expert", "width")
    return jax.shard_map(body, mesh=mesh, in_specs=in_specs, out_specs=out_specs, check_vma=False)
```

```python
import functools

import jax
import jax.numpy as jnp
from jax import lax
from jax.experimental import pallas as pl
from jax.experimental.pallas import tpu as pltpu
from jax.sharding import PartitionSpec as P

SEND = 2
LANES = 128
VMEM = pl.BlockSpec(memory_space=pltpu.VMEM)
HBM = pl.BlockSpec(memory_space=pltpu.HBM)
F32 = jnp.float32
BF16 = jnp.bfloat16


def params(mib):
    return pltpu.CompilerParams(vmem_limit_bytes=mib << 20)


def hint(micros):
    return pl.CostEstimate(flops=micros * 10**9, bytes_accessed=0, transcendentals=0)


def split_rows(ref, value):
    piece = ref.shape[2]
    pieces = value.shape[1] // piece
    for i in range(ref.shape[0]):
        e, u = divmod(i, pieces)
        ref[i] = value[e * SEND : (e + 1) * SEND, u * piece : (u + 1) * piece]


def join_rows(ref, u, pieces):
    return jnp.concatenate([ref[i] for i in range(u, ref.shape[0], pieces)], axis=0)


def slots_kernel(ids_hbm, weight_hbm, tokens_hbm, taken_ref, coeff_ref, tokens_ref, ids_ref, weight_ref, sems):
    copies = [
        pltpu.make_async_copy(source, target, sems.at[i])
        for i, (source, target) in enumerate(
            ((ids_hbm, ids_ref), (weight_hbm, weight_ref), (tokens_hbm, tokens_ref))
        )
    ]
    for copy in copies:
        copy.start()
    slots, rows = coeff_ref.shape
    slot = lax.broadcasted_iota(jnp.int32, (slots, rows), 0)
    expert, rank = slot // SEND, slot % SEND
    earlier = lax.broadcasted_iota(jnp.int32, (rows, rows), 0) < lax.broadcasted_iota(
        jnp.int32, (rows, rows), 1
    )
    hits = jnp.zeros((slots, rows), F32)
    weight = jnp.zeros((slots, rows), F32)
    copies[0].wait()
    copies[1].wait()
    for k in range(ids_ref.shape[0]):
        hit = ids_ref[k : k + 1, :] == expert
        hits = jnp.where(hit, 1.0, hits)
        weight = jnp.where(hit, weight_ref[k : k + 1, :], weight)
    ranking = jnp.dot(hits.astype(BF16), earlier.astype(BF16), preferred_element_type=F32)
    taken = jnp.logical_and(hits > 0.0, ranking == rank.astype(F32))
    coeff_ref[...] = jnp.where(taken, weight, 0.0)
    taken_ref[...] = jnp.where(taken, 1.0, 0.0).astype(BF16)
    copies[2].wait()


def select_kernel(taken_ref, tokens_ref, outgoing_ref):
    split_rows(
        outgoing_ref,
        jnp.dot(taken_ref[...], tokens_ref[...], preferred_element_type=F32).astype(BF16),
    )


def owned(d, features, pieces):
    width = lax.axis_size("width")
    owner = lax.rem(lax.axis_index("width") + width - d, width)
    if pieces == 1:
        return [pl.ds(pl.multiple_of(owner * features, features), features)]
    piece = features // pieces
    return [
        pl.ds(pl.multiple_of(u * features + owner * piece, piece), piece) for u in range(pieces)
    ]


def gate_up(rows_ref, gate_ref, up_ref, d, pieces, gate, up):
    for u, block in enumerate(owned(d, rows_ref.shape[2] * pieces, pieces)):
        x = join_rows(rows_ref, u, pieces)
        gate += jnp.dot(x, gate_ref[0, block, :], preferred_element_type=F32)
        up += jnp.dot(x, up_ref[0, block, :], preferred_element_type=F32)
    return gate, up


def own_kernel(pieces, rows_ref, gate_ref, up_ref, down_ref, gate_out, up_out):
    del down_ref
    gate_out[...], up_out[...] = gate_up(rows_ref, gate_ref, up_ref, 0, pieces, 0.0, 0.0)


def down_part(hidden, down_ref, d, pieces, part_ref):
    features = part_ref.shape[1]
    piece = features // pieces
    for u, block in enumerate(owned(d, features, pieces)):
        part_ref[:, u * piece : (u + 1) * piece] = lax.dot_general(
            hidden, down_ref[0, block, :], (((1,), (1,)), ((), ())), preferred_element_type=F32
        ).astype(BF16)


def others_kernel(others, pieces, *refs):
    rows = refs[:others]
    gate_in, up_in, gate_ref, up_ref, down_ref = refs[others : others + 5]
    hidden_ref = refs[others + 5]
    parts = refs[others + 6 :]
    gate, up = gate_in[...], up_in[...]
    for d in range(others):
        gate, up = gate_up(rows[d], gate_ref, up_ref, d + 1, pieces, gate, up)
    hidden = (gate / (1.0 + jnp.exp(-gate)) * up).astype(BF16)
    hidden_ref[...] = hidden
    for d in range(others):
        down_part(hidden, down_ref, d + 1, pieces, parts[d])


def own_part_kernel(pieces, hidden_ref, down_ref, part_ref):
    down_part(hidden_ref[...], down_ref, 0, pieces, part_ref)


def sum_kernel(*refs):
    summed = refs[0][...].astype(F32)
    for part in refs[1:-1]:
        summed += part[...].astype(F32)
    split_rows(refs[-1], summed.astype(BF16))


def combine_kernel(pieces, coeff_ref, returned_ref, mixed_hbm, mixed_ref, sems):
    coeff = coeff_ref[...]
    high = coeff.astype(BF16)
    low = (coeff - high.astype(F32)).astype(BF16)
    dims = (((0,), (0,)), ((), ()))
    piece = returned_ref.shape[2]
    copies = []
    for u in range(pieces):
        returned = join_rows(returned_ref, u, pieces)
        block = (slice(None), pl.ds(u * piece, piece))
        mixed_ref[block] = (
            lax.dot_general(high, returned, dims, preferred_element_type=F32)
            + lax.dot_general(low, returned, dims, preferred_element_type=F32)
        ).astype(BF16)
        copies.append(pltpu.make_async_copy(mixed_ref.at[block], mixed_hbm.at[block], sems.at[u]))
        copies[-1].start()
    for copy in copies:
        copy.wait()


def body(tokens, expert_ids, route_weight, gate_weight, up_weight, down_weight):
    holders, width = lax.axis_size("expert"), lax.axis_size("width")
    rows, features = tokens.shape
    top = expert_ids.shape[1]
    hidden_units = gate_weight.shape[2]
    slots = holders * SEND
    pieces = width if features % (width * LANES) == 0 else 1
    sent = (holders * pieces, SEND, features // pieces)
    shape = jax.ShapeDtypeStruct

    ids, weights, tokens = (
        pltpu.with_memory_space_constraint(x, pltpu.HBM)
        for x in (expert_ids.T, route_weight.T, tokens)
    )
    taken, coeff, tokens = pl.pallas_call(
        slots_kernel,
        out_shape=(
            shape((slots, rows), BF16),
            shape((slots, rows), F32),
            shape((rows, features), BF16),
        ),
        in_specs=[HBM] * 3,
        out_specs=[VMEM] * 3,
        scratch_shapes=[
            pltpu.VMEM((top, rows), jnp.int32),
            pltpu.VMEM((top, rows), F32),
            pltpu.SemaphoreType.DMA((3,)),
        ],
        compiler_params=params(8),
        name="slots",
    )(ids, weights, tokens)
    outgoing = pl.pallas_call(
        select_kernel,
        out_shape=shape(sent, BF16),
        in_specs=[VMEM] * 2,
        out_specs=VMEM,
        compiler_params=params(8),
        cost_estimate=hint(40),
        name="select",
    )(taken, tokens)

    def exchange(x):
        axes = "expert" if pieces == 1 else ("expert", "width")
        return lax.all_to_all(x, axes, split_axis=0, concat_axis=0, tiled=True)

    def shifted(x, d):
        return lax.ppermute(x, "width", [(i, (i + d) % width) for i in range(width)])

    arrived = exchange(outgoing)
    others = [shifted(arrived, d) for d in range(1, width)]
    gate_vmem, up_vmem, down_vmem = (
        pltpu.with_memory_space_constraint(w, pltpu.VMEM)
        for w in (gate_weight, up_weight, down_weight)
    )
    gate, up = pl.pallas_call(
        functools.partial(own_kernel, pieces),
        out_shape=[shape((slots, hidden_units), F32)] * 2,
        in_specs=[VMEM] * 4,
        out_specs=[VMEM] * 2,
        compiler_params=params(20),
        cost_estimate=hint(2),
        name="own",
    )(arrived, gate_vmem, up_vmem, down_vmem)
    hidden, *parts = pl.pallas_call(
        functools.partial(others_kernel, width - 1, pieces),
        out_shape=[shape((slots, hidden_units), BF16)]
        + [shape((slots, features), BF16)] * (width - 1),
        in_specs=[VMEM] * (width + 4),
        out_specs=[VMEM] * width,
        compiler_params=params(24),
        cost_estimate=hint(2),
        name="others",
    )(*others, gate, up, gate_vmem, up_vmem, down_vmem)
    received = [shifted(part, d + 1) for d, part in enumerate(reversed(parts))]
    part = pl.pallas_call(
        functools.partial(own_part_kernel, pieces),
        out_shape=shape((slots, features), BF16),
        in_specs=[VMEM] * 2,
        out_specs=VMEM,
        compiler_params=params(20),
        cost_estimate=hint(2),
        name="own_part",
    )(hidden, down_vmem)
    summed = pl.pallas_call(
        sum_kernel,
        out_shape=shape(sent, BF16),
        in_specs=[VMEM] * width,
        out_specs=VMEM,
        compiler_params=params(8),
        name="sum",
    )(part, *received)
    returned = exchange(summed)
    return pl.pallas_call(
        functools.partial(combine_kernel, pieces),
        out_shape=shape((rows, features), BF16),
        in_specs=[VMEM] * 2,
        out_specs=HBM,
        scratch_shapes=[pltpu.VMEM((rows, features), BF16), pltpu.SemaphoreType.DMA((pieces,))],
        compiler_params=params(8),
        name="combine",
    )(coeff, returned)


def solution(mesh):
    in_specs = (
        P("expert", "width"),
        P("expert", None),
        P("expert", None),
        P("expert", None, "width"),
        P("expert", None, "width"),
        P("expert", None, "width"),
    )
    out_specs = P("expert", "width")
    return jax.shard_map(body, mesh=mesh, in_specs=in_specs, out_specs=out_specs, check_vma=False)
```

```python
import functools

import jax
import jax.numpy as jnp
from jax import lax
from jax.experimental import pallas as pl
from jax.experimental.pallas import tpu as pltpu
from jax.sharding import PartitionSpec as P

SEND = 2
LANES = 128
STEPS = (512, 384, 256, 128)
VMEM = pl.BlockSpec(memory_space=pltpu.VMEM)
HBM = pl.BlockSpec(memory_space=pltpu.HBM)
F32 = jnp.float32
BF16 = jnp.bfloat16


def params(mib):
    return pltpu.CompilerParams(vmem_limit_bytes=mib << 20)


def hint(micros):
    return pl.CostEstimate(flops=micros * 10**9, bytes_accessed=0, transcendentals=0)


def split_rows(ref, value):
    piece = ref.shape[2]
    pieces = value.shape[1] // piece
    for i in range(ref.shape[0]):
        e, u = divmod(i, pieces)
        ref[i] = value[e * SEND : (e + 1) * SEND, u * piece : (u + 1) * piece]


def join_rows(ref, u, pieces):
    return jnp.concatenate([ref[i] for i in range(u, ref.shape[0], pieces)], axis=0)


def slots_kernel(ids_hbm, weight_hbm, tokens_hbm, taken_ref, coeff_ref, tokens_ref, ids_ref, weight_ref, sems):
    copies = [
        pltpu.make_async_copy(source, target, sems.at[i])
        for i, (source, target) in enumerate(
            ((ids_hbm, ids_ref), (weight_hbm, weight_ref), (tokens_hbm, tokens_ref))
        )
    ]
    for copy in copies:
        copy.start()
    slots, rows = coeff_ref.shape
    slot = lax.broadcasted_iota(jnp.int32, (slots, rows), 0)
    expert, rank = slot // SEND, slot % SEND
    earlier = lax.broadcasted_iota(jnp.int32, (rows, rows), 0) < lax.broadcasted_iota(
        jnp.int32, (rows, rows), 1
    )
    hits = jnp.zeros((slots, rows), F32)
    weight = jnp.zeros((slots, rows), F32)
    copies[0].wait()
    copies[1].wait()
    for k in range(ids_ref.shape[0]):
        hit = ids_ref[k : k + 1, :] == expert
        hits = jnp.where(hit, 1.0, hits)
        weight = jnp.where(hit, weight_ref[k : k + 1, :], weight)
    ranking = jnp.dot(hits.astype(BF16), earlier.astype(BF16), preferred_element_type=F32)
    taken = jnp.logical_and(hits > 0.0, ranking == rank.astype(F32))
    coeff_ref[...] = jnp.where(taken, weight, 0.0)
    taken_ref[...] = jnp.where(taken, 1.0, 0.0).astype(BF16)
    copies[2].wait()


def select_kernel(taken_ref, tokens_ref, outgoing_ref):
    split_rows(
        outgoing_ref,
        jnp.dot(taken_ref[...], tokens_ref[...], preferred_element_type=F32).astype(BF16),
    )


def owned(d, features, pieces):
    width = lax.axis_size("width")
    owner = lax.rem(lax.axis_index("width") + width - d, width)
    if pieces == 1:
        return [pl.ds(pl.multiple_of(owner * features, features), features)]
    piece = features // pieces
    return [
        pl.ds(pl.multiple_of(u * features + owner * piece, piece), piece) for u in range(pieces)
    ]


def gate_up(rows_ref, gate_ref, up_ref, d, pieces, gate, up):
    for u, block in enumerate(owned(d, rows_ref.shape[2] * pieces, pieces)):
        x = join_rows(rows_ref, u, pieces)
        gate += jnp.dot(x, gate_ref[0, block, :], preferred_element_type=F32)
        up += jnp.dot(x, up_ref[0, block, :], preferred_element_type=F32)
    return gate, up


def own_kernel(others, pieces, rows_ref, coeff_ref, gate_ref, up_ref, down_ref, *outs):
    gate_out, up_out, split_ref = outs[:3]
    turned = outs[3:]
    coeff = coeff_ref[...].T
    high = coeff.astype(BF16)
    rows = coeff.shape[0]
    split_ref[:rows, :] = high
    split_ref[rows:, :] = (coeff - high.astype(F32)).astype(BF16)
    piece = rows_ref.shape[2]
    features = piece * pieces
    step = next((n for n in STEPS if piece % n == 0), piece)
    own = owned(0, features, pieces)
    theirs = [owned(d + 1, features, pieces) for d in range(others)]
    gate = up = 0.0
    for u in range(pieces):
        x = join_rows(rows_ref, u, pieces)
        for i in range(0, piece, step):
            block = pl.ds(pl.multiple_of(own[u].start + i, step), step)
            gate += jnp.dot(x[:, i : i + step], gate_ref[0, block, :], preferred_element_type=F32)
            up += jnp.dot(x[:, i : i + step], up_ref[0, block, :], preferred_element_type=F32)
            at = u * piece + i
            for d in range(others):
                block = pl.ds(pl.multiple_of(theirs[d][u].start + i, step), step)
                turned[d][:, at : at + step] = down_ref[0, block, :].T
    gate_out[...] = gate
    up_out[...] = up


def down_part(hidden, down_ref, d, pieces, part_ref):
    features = part_ref.shape[1]
    piece = features // pieces
    for u, block in enumerate(owned(d, features, pieces)):
        part_ref[:, u * piece : (u + 1) * piece] = lax.dot_general(
            hidden, down_ref[0, block, :], (((1,), (1,)), ((), ())), preferred_element_type=F32
        ).astype(BF16)


def others_kernel(others, pieces, *refs):
    rows = refs[:others]
    turned = refs[others : 2 * others]
    gate_in, up_in, gate_ref, up_ref, hidden_ref = refs[2 * others : 2 * others + 5]
    parts = refs[2 * others + 5 :]
    gate, up = gate_in[...], up_in[...]
    for d in range(others):
        gate, up = gate_up(rows[d], gate_ref, up_ref, d + 1, pieces, gate, up)
    hidden = (gate / (1.0 + jnp.exp(-gate)) * up).astype(BF16)
    hidden_ref[...] = hidden
    for d in range(others):
        parts[d][...] = jnp.dot(hidden, turned[d][...], preferred_element_type=F32).astype(BF16)


def own_part_kernel(pieces, hidden_ref, down_ref, part_ref):
    down_part(hidden_ref[...], down_ref, 0, pieces, part_ref)


def sum_kernel(*refs):
    summed = refs[0][...].astype(F32)
    for part in refs[1:-1]:
        summed += part[...].astype(F32)
    split_rows(refs[-1], summed.astype(BF16))


def combine_kernel(pieces, coeff_ref, returned_ref, mixed_hbm, mixed_ref, sems):
    coeff = coeff_ref[...]
    rows = mixed_ref.shape[0]
    piece = returned_ref.shape[2]
    copies = []
    for u in range(pieces):
        returned = join_rows(returned_ref, u, pieces)
        block = (slice(None), pl.ds(u * piece, piece))
        mixed = jnp.dot(coeff, returned, preferred_element_type=F32)
        mixed_ref[block] = (mixed[:rows] + mixed[rows:]).astype(BF16)
        copies.append(pltpu.make_async_copy(mixed_ref.at[block], mixed_hbm.at[block], sems.at[u]))
        copies[-1].start()
    for copy in copies:
        copy.wait()


def body(tokens, expert_ids, route_weight, gate_weight, up_weight, down_weight):
    holders, width = lax.axis_size("expert"), lax.axis_size("width")
    rows, features = tokens.shape
    top = expert_ids.shape[1]
    hidden_units = gate_weight.shape[2]
    slots = holders * SEND
    pieces = width if features % (width * LANES) == 0 else 1
    sent = (holders * pieces, SEND, features // pieces)
    shape = jax.ShapeDtypeStruct

    ids, weights, tokens = (
        pltpu.with_memory_space_constraint(x, pltpu.HBM)
        for x in (expert_ids.T, route_weight.T, tokens)
    )
    taken, coeff, tokens = pl.pallas_call(
        slots_kernel,
        out_shape=(
            shape((slots, rows), BF16),
            shape((slots, rows), F32),
            shape((rows, features), BF16),
        ),
        in_specs=[HBM] * 3,
        out_specs=[VMEM] * 3,
        scratch_shapes=[
            pltpu.VMEM((top, rows), jnp.int32),
            pltpu.VMEM((top, rows), F32),
            pltpu.SemaphoreType.DMA((3,)),
        ],
        compiler_params=params(8),
        name="slots",
    )(ids, weights, tokens)
    outgoing = pl.pallas_call(
        select_kernel,
        out_shape=shape(sent, BF16),
        in_specs=[VMEM] * 2,
        out_specs=VMEM,
        compiler_params=params(8),
        cost_estimate=hint(40),
        name="select",
    )(taken, tokens)

    def exchange(x):
        axes = "expert" if pieces == 1 else ("expert", "width")
        return lax.all_to_all(x, axes, split_axis=0, concat_axis=0, tiled=True)

    def shifted(x, d):
        return lax.ppermute(x, "width", [(i, (i + d) % width) for i in range(width)])

    arrived = exchange(outgoing)
    others = [shifted(arrived, d) for d in range(1, width)]
    gate_vmem, up_vmem, down_vmem = (
        pltpu.with_memory_space_constraint(w, pltpu.VMEM)
        for w in (gate_weight, up_weight, down_weight)
    )
    gate, up, coeff, *turned = pl.pallas_call(
        functools.partial(own_kernel, width - 1, pieces),
        out_shape=[shape((slots, hidden_units), F32)] * 2
        + [shape((2 * rows, slots), BF16)]
        + [shape((hidden_units, features), BF16)] * (width - 1),
        in_specs=[VMEM] * 5,
        out_specs=[VMEM] * (width + 2),
        compiler_params=params(20),
        cost_estimate=hint(2),
        name="own",
    )(arrived, coeff, gate_vmem, up_vmem, down_vmem)
    hidden, *parts = pl.pallas_call(
        functools.partial(others_kernel, width - 1, pieces),
        out_shape=[shape((slots, hidden_units), BF16)]
        + [shape((slots, features), BF16)] * (width - 1),
        in_specs=[VMEM] * (2 * width + 2),
        out_specs=[VMEM] * width,
        compiler_params=params(24),
        cost_estimate=hint(2),
        name="others",
    )(*others, *turned, gate, up, gate_vmem, up_vmem)
    received = [shifted(part, d + 1) for d, part in enumerate(reversed(parts))]
    part = pl.pallas_call(
        functools.partial(own_part_kernel, pieces),
        out_shape=shape((slots, features), BF16),
        in_specs=[VMEM] * 2,
        out_specs=VMEM,
        compiler_params=params(20),
        cost_estimate=hint(2),
        name="own_part",
    )(hidden, down_vmem)
    summed = pl.pallas_call(
        sum_kernel,
        out_shape=shape(sent, BF16),
        in_specs=[VMEM] * width,
        out_specs=VMEM,
        compiler_params=params(8),
        name="sum",
    )(part, *received)
    returned = exchange(summed)
    return pl.pallas_call(
        functools.partial(combine_kernel, pieces),
        out_shape=shape((rows, features), BF16),
        in_specs=[VMEM] * 2,
        out_specs=HBM,
        scratch_shapes=[pltpu.VMEM((rows, features), BF16), pltpu.SemaphoreType.DMA((pieces,))],
        compiler_params=params(8),
        name="combine",
    )(coeff, returned)


def solution(mesh):
    in_specs = (
        P("expert", "width"),
        P("expert", None),
        P("expert", None),
        P("expert", None, "width"),
        P("expert", None, "width"),
        P("expert", None, "width"),
    )
    out_specs = P("expert", "width")
    return jax.shard_map(body, mesh=mesh, in_specs=in_specs, out_specs=out_specs, check_vma=False)
```
